32 devices in a mesh: row: 4 (over y, x), col: 8 (over z, core).
Axes of the slice: x: 2, y: 2, z: 4, core: 2. Of those that a mesh axis runs over, the one named last changes fastest.
Arguments:
- dense_in: bfloat16 [512, 28672], P('col', 'row'), may hold values from -6 to 6
- pruned_in: bfloat16 [512, 28672], P('col', 'row'), may hold values from -6 to 6
- weight: bfloat16 [28672, 8192], P('row', 'col'), may hold values from -0.03125 to 0.03125
- keep_bits: int32 [512, 28672], P('col', 'row'), may hold values from 0 to 65535
Outputs:
- gram_tile: float32 [8192, 8192], P('row', 'col')
- cross_tile: float32 [8192, 8192], P('row', 'col')
The draws below stay inside these ranges and needn't reach their ends.
Inputs may be any that keep to these rules, and one draw needn't show every extreme that they name: `keep_bits`: each word holds 16 independent flags, each 1 with probability one half.
All inputs are finite; a program needn't handle non-finite values.
Results may differ from the reference program's by a relative error of at most 0.0039.
Values may be sent and summed in bfloat16 or wider, within the bound.
A program may use at most 128 MiB of HBM per device.

```python
import jax
import jax.numpy as jnp
from jax import lax

D = 8192
FF = 28672
TOKENS = 512
WORDS = 512
N_COL = 8


def place_ends(result, rng, low, top_value):
    extent = result.shape
    index_at = [jax.random.randint(jax.random.fold_in(rng, axis), (), 0, extent[axis]) for axis in range(len(extent))]
    result = result.at[tuple(index_at)].set(low)
    longest = extent.index(max(extent))
    index_at[longest] = (index_at[longest] + 1) % extent[longest]
    return result.at[tuple(index_at)].set(top_value)


def steps_of(own_key, extent, shards, low, largest):
    level = 1.0
    for axis_at, parts in shards:
        draws = jax.random.uniform(jax.random.fold_in(jax.random.fold_in(own_key, 6), axis_at), (parts,), jnp.float32, low / len(shards), largest / len(shards))
        level = level * jnp.repeat(jnp.exp(draws), extent[axis_at] // parts).reshape((-1,) + (1,) * (len(extent) - 1 - axis_at))
    return level


def gaussian(stream_key, shape, spread, reach, shards=(), kind=jnp.bfloat16):
    factor_of = steps_of(stream_key, shape, shards, -0.22, 0.18) if shards else 1.0
    array = jax.random.normal(stream_key, shape, jnp.float32) * spread * factor_of
    return jnp.minimum(jnp.maximum(array, -reach), reach).astype(kind)


def setup_inputs(seed: int = 0) -> dict:
    arg_keys = jax.random.split(jax.random.key(seed), 5)
    dense_in = gaussian(arg_keys[0], (TOKENS, FF), 1.0, 6.0, ((0, 8), (1, 4)))
    pruned_in = gaussian(arg_keys[1], (TOKENS, FF), 1.0, 6.0, ((0, 8), (1, 4)))
    weight = gaussian(arg_keys[2], (FF, D), FF ** -0.5, 0.03125, ((0, 4), (1, 8)))
    keep_bits = place_ends(jax.random.randint(arg_keys[3], (WORDS, FF), 0, 65536), jax.random.fold_in(arg_keys[3], 1), 0, 65535).astype(jnp.int32)
    return {"dense_in": dense_in, "pruned_in": pruned_in, "weight": weight, "keep_bits": keep_bits}


def unpack_block(word_block, columns):
    shifts = jnp.arange(16, dtype=jnp.int32)
    flag_bits = jnp.right_shift(word_block[:, None, :], shifts[None, :, None]) & 1
    return flag_bits.reshape(word_block.shape[0] * 16, word_block.shape[1])[:columns]


def reference(dense_in, pruned_in, weight, keep_bits):
    columns = D // N_COL
    per_block = keep_bits.shape[0] // N_COL
    keep_flags = jnp.concatenate([unpack_block(keep_bits[index * per_block:(index + 1) * per_block], columns) for index in range(N_COL)], 0)
    pruned_w = jnp.where(keep_flags.T == 1, weight, jnp.zeros_like(weight))
    dense_out = jnp.dot(dense_in, weight, preferred_element_type=jnp.float32)
    pruned_out = jnp.dot(pruned_in, pruned_w, preferred_element_type=jnp.float32)
    pruned_b = pruned_out.astype(jnp.bfloat16)
    difference = (dense_out - pruned_out).astype(jnp.bfloat16)
    dims = (((0,), (0,)), ((), ()))
    gram_tile = lax.dot_general(pruned_b, pruned_b, dims, preferred_element_type=jnp.float32) / TOKENS
    cross_tile = lax.dot_general(difference, pruned_b, dims, preferred_element_type=jnp.float32) / TOKENS
    return gram_tile, cross_tile
```

```python
import functools

import jax
import jax.numpy as jnp
from jax import lax
from jax.experimental import pallas as pl
from jax.experimental.pallas import tpu as pltpu
from jax.sharding import PartitionSpec as P

MESH = pl.DeviceIdType.MESH
CORES = 2
FLAG_BITS = 16
HALF_BITS = 8


def block_of(size, choices):
    for choice in choices:
        if size % choice == 0:
            return choice
    return size


def gather_kernel(
    n_row, n_col,
    pruned_in, dense_in, weight, keep,
    cols, panels,
    xs, ws, flags, pick, part, heard, piece,
    weight_sem, keep_sem, own_sem, x_recv, left_send, right_send, mate_send,
    sum_send, sum_recv, col_send, col_recv, col_own,
    panel_send, panel_recv, panel_own, pair_send, pair_recv,
):
    rows, depth = pruned_in.shape
    features = weight.shape[1]
    words = keep.shape[0]
    line = n_col // CORES
    per_row = n_col // n_row
    together = CORES * rows
    share = together // n_row
    row, col = lax.axis_index("row"), lax.axis_index("col")
    z, core = col // CORES, lax.rem(col, CORES)
    other = 1 - core
    mate = (row, z * CORES + other)
    home = col // per_row
    slot = lax.rem(col, per_row)

    barrier = pltpu.get_barrier_semaphore()
    for d in range(n_row):
        for e in range(n_col):
            if d or e:
                peer = (lax.rem(row + d, n_row), lax.rem(col + e, n_col))
                pl.semaphore_signal(barrier, inc=1, device_id=peer, device_id_type=MESH)

    chunk = block_of(depth, (512, 256, 128))
    chunks = depth // chunk

    def load_chunk(i):
        at = pl.ds(pl.multiple_of(i * chunk, chunk), chunk)
        return pltpu.make_async_copy(weight.at[at], ws.at[1, at], weight_sem.at[i])

    load_keep = pltpu.make_async_copy(keep, flags, keep_sem)
    load_keep.start()

    @pl.loop(0, chunks)
    def _(i):
        load_chunk(i).start()

    sources = (pruned_in, dense_in)

    def half(q, which):
        return pl.ds(pl.multiple_of(which * rows, rows), rows)

    def own_copy(m):
        return pltpu.make_async_copy(sources[m], xs.at[m, z, half(z, core)], own_sem.at[m])

    for m in range(2):
        own_copy(m).start()

    def x_copy(m, q, which, source, target, send):
        return pltpu.make_async_remote_copy(
            src_ref=source,
            dst_ref=xs.at[m, q, half(q, which)],
            send_sem=send,
            recv_sem=x_recv.at[m, q, which],
            device_id=target,
            device_id_type=MESH,
        )

    def block(m, q):
        return xs.at[m, q, half(q, core)]

    def to_left(m, q, source):
        return x_copy(m, q, core, source, (row, col - CORES), left_send.at[m, q])

    def to_right(m, q, source):
        return x_copy(m, q, core, source, (row, col + CORES), right_send.at[m, q])

    def to_mate(m, q, source):
        return x_copy(m, q, core, source, mate, mate_send.at[m, q])

    pl.semaphore_wait(barrier, n_row * n_col - 1)
    for m in range(2):
        @pl.when(z > 0)
        def _():
            to_left(m, z, sources[m]).start()

        @pl.when(z < line - 1)
        def _():
            to_right(m, z, sources[m]).start()

    for m in range(2):
        to_mate(m, z, sources[m]).start()

    w_at = lax.broadcasted_iota(jnp.int32, (2 * words, features), 0)
    f_at = lax.broadcasted_iota(jnp.int32, (2 * words, features), 1)
    high = jnp.where(w_at >= words, 1, 0)
    match = (w_at - high * words == f_at // FLAG_BITS) & (high == lax.rem(f_at, FLAG_BITS) // HALF_BITS)
    pick[...] = jnp.where(match, 1.0, 0.0).astype(jnp.bfloat16)
    lane = lax.broadcasted_iota(jnp.int32, (1, features), 1)
    bit = jnp.left_shift(jnp.ones_like(lane), lax.rem(lane, HALF_BITS))
    tile = block_of(chunk, (256, 128))
    load_keep.wait()

    @pl.loop(0, chunks)
    def _(i):
        load_chunk(i).wait()

        @pl.loop(0, chunk // tile)
        def _(j):
            start = pl.multiple_of(i * chunk + j * tile, tile)
            word = flags[:, pl.ds(start, tile)]
            low = (word & 255).astype(jnp.float32)
            top = (jnp.right_shift(word, HALF_BITS) & 255).astype(jnp.float32)
            halves = jnp.concatenate([low, top], 0).T.astype(jnp.bfloat16)
            spread = jnp.dot(halves, pick[...], preferred_element_type=jnp.float32)
            kept = jnp.where((spread.astype(jnp.int32) & bit) != 0, 1.0, 0.0)
            ws[0, pl.ds(start, tile), :] = ws[1, pl.ds(start, tile), :] * kept.astype(jnp.bfloat16)

    def position(s, side):
        return z + s * (1 - 2 * side)

    def present(s, side, q):
        return (q >= 0) & (q < line) & ((s > 0) | (side == 0))

    def arrive(m, s):
        @pl.loop(0, 2)
        def _(side):
            q = position(s, side)

            @pl.when(present(s, side, q) & (s > 0))
            def _():
                to_mate(m, q, block(m, q)).wait_recv()

                @pl.when((side == 0) & (z > 0))
                def _():
                    to_left(m, q, block(m, q)).start()

                @pl.when((side == 1) & (z < line - 1))
                def _():
                    to_right(m, q, block(m, q)).start()

                to_mate(m, q, block(m, q)).start()

    def sum_copy(m, q, d):
        target = lax.rem(row + d, n_row)
        at = pl.ds(pl.multiple_of(target * share, share), share)
        return pltpu.make_async_remote_copy(
            src_ref=part.at[m, q, at],
            dst_ref=heard.at[m, q, d - 1],
            send_sem=sum_send.at[m, q, d - 1],
            recv_sem=sum_recv.at[m, q, d - 1],
            device_id=(target, col),
            device_id_type=MESH,
        )

    wide = block_of(features, (512, 256, 128))

    def multiply(m, s):
        @pl.loop(0, 2)
        def _(side):
            q = position(s, side)

            @pl.when(present(s, side, q))
            def _():
                x_copy(m, q, other, block(m, q), mate, mate_send.at[m, q]).wait_recv()

                @pl.loop(0, features // wide)
                def _(n):
                    at = pl.ds(pl.multiple_of(n * wide, wide), wide)
                    part[m, q, :, at] = jnp.dot(xs[m, q], ws[m, :, at], preferred_element_type=jnp.float32)

                @pl.when(m == 1)
                def _():
                    part[1, q] = part[1, q] - part[0, q]

                for d in range(1, n_row):
                    sum_copy(m, q, d).start()

    def token_rows(q, which):
        return pl.ds(pl.multiple_of(q * together + which * share, share), share)

    def slot_columns(j):
        return pl.ds(pl.multiple_of(j * features, features), features)

    def col_copy(q, d):
        return pltpu.make_async_remote_copy(
            src_ref=piece.at[0, q],
            dst_ref=cols.at[token_rows(q, row)],
            send_sem=col_send.at[q, d - 1],
            recv_sem=col_recv.at[q, d - 1],
            device_id=(lax.rem(row + d, n_row), col),
            device_id_type=MESH,
        )

    def col_local(q):
        return pltpu.make_async_copy(piece.at[0, q], cols.at[token_rows(q, row)], col_own.at[q])

    def panel_copy(m, q, j, source_row, at):
        return pltpu.make_async_remote_copy(
            src_ref=piece.at[m, q],
            dst_ref=panels.at[m, token_rows(q, source_row), slot_columns(j)],
            send_sem=panel_send.at[m, q, at],
            recv_sem=panel_recv.at[m, q, j, source_row],
            device_id=(home, at * CORES + core),
            device_id_type=MESH,
        )

    def panel_local(m, q):
        return pltpu.make_async_copy(
            piece.at[m, q], panels.at[m, token_rows(q, row), slot_columns(slot)], panel_own.at[m, q]
        )

    def is_self(at):
        return (at == z) & (row == home)

    def settle(m, s):
        @pl.loop(0, 2)
        def _(side):
            q = position(s, side)

            @pl.when(present(s, side, q))
            def _():
                total = part[m, q, pl.ds(pl.multiple_of(row * share, share), share), :]
                for d in range(1, n_row):
                    sum_copy(m, q, d).wait_recv()
                    total = total + heard[m, q, d - 1]
                piece[m, q] = total.astype(jnp.bfloat16)

                @pl.loop(0, line)
                def _(at):
                    @pl.when(is_self(at))
                    def _():
                        panel_local(m, q).start()

                    @pl.when(jnp.logical_not(is_self(at)))
                    def _():
                        panel_copy(m, q, slot, row, at).start()

                @pl.when(m == 0)
                def _():
                    col_local(q).start()
                    for d in range(1, n_row):
                        col_copy(q, d).start()

    for m in range(2):
        own_copy(m).wait()

    @pl.loop(0, 2 * line)
    def _(t):
        s, m = t // 2, lax.rem(t, 2)
        arrive(m, s)
        multiply(m, s)

        @pl.when(t > 0)
        def _():
            settle(1 - m, (t - 1) // 2)

    settle(1, line - 1)

    def comes_here(j):
        return lax.rem(row * per_row + j, CORES) == core

    def panel_rows(q):
        return pl.ds(pl.multiple_of(q * together, together), together)

    def pair_copy(m, q, j):
        part_of = panels.at[m, panel_rows(q), slot_columns(j)]
        return pltpu.make_async_remote_copy(
            src_ref=part_of,
            dst_ref=part_of,
            send_sem=pair_send.at[m, q, j],
            recv_sem=pair_recv.at[m, q, j],
            device_id=mate,
            device_id_type=MESH,
        )

    @pl.loop(0, 2 * line)
    def _(t):
        s, m = t // 2, lax.rem(t, 2)

        @pl.loop(0, 2)
        def _(side):
            for j in range(per_row):
                origin = (row * per_row + j) // CORES
                q = origin + s * (1 - 2 * side)

                @pl.when(present(s, side, q) & comes_here(j))
                def _():
                    for source_row in range(n_row):
                        here = (origin == z) & (row == source_row)

                        @pl.when(here)
                        def _():
                            panel_local(m, q).wait()

                        @pl.when(jnp.logical_not(here))
                        def _():
                            panel_copy(m, q, j, source_row, z).wait_recv()

                    pair_copy(m, q, j).start()

    @pl.loop(0, line)
    def _(q):
        col_local(q).wait()
        for d in range(1, n_row):
            col_copy(q, d).wait_recv()
            col_copy(q, d).wait_send()
        for m in range(2):
            for j in range(per_row):
                @pl.when(comes_here(j))
                def _():
                    pair_copy(m, q, j).wait_send()

                @pl.when(jnp.logical_not(comes_here(j)))
                def _():
                    pair_copy(m, q, j).wait_recv()

            @pl.loop(0, line)
            def _(at):
                @pl.when(jnp.logical_not(is_self(at)))
                def _():
                    panel_copy(m, q, slot, row, at).wait_send()

            for d in range(1, n_row):
                sum_copy(m, q, d).wait_send()
            to_mate(m, q, block(m, q)).wait_send()

            @pl.when((z > 0) & (q >= z))
            def _():
                to_left(m, q, block(m, q)).wait_send()

            @pl.when((z < line - 1) & (q <= z))
            def _():
                to_right(m, q, block(m, q)).wait_send()


def gather(pruned_in, dense_in, weight, keep_bits):
    n_row, n_col = lax.axis_size("row"), lax.axis_size("col")
    rows, depth = pruned_in.shape
    features = weight.shape[1]
    words = keep_bits.shape[0]
    line, per_row = n_col // CORES, n_col // n_row
    together, tokens = CORES * rows, n_col * rows
    share = together // n_row
    dma = pltpu.SemaphoreType.DMA
    chunks = depth // block_of(depth, (512, 256, 128))
    anywhere = pl.BlockSpec(memory_space=pl.ANY)
    return pl.pallas_call(
        functools.partial(gather_kernel, n_row, n_col),
        out_shape=(
            jax.ShapeDtypeStruct((tokens, features), jnp.bfloat16),
            jax.ShapeDtypeStruct((2, tokens, per_row * features), jnp.bfloat16),
        ),
        in_specs=[anywhere] * 4,
        out_specs=(anywhere, anywhere),
        scratch_shapes=[
            pltpu.VMEM((2, line, together, depth), jnp.bfloat16),
            pltpu.VMEM((2, depth, features), jnp.bfloat16),
            pltpu.VMEM((words, depth), jnp.int32),
            pltpu.VMEM((2 * words, features), jnp.bfloat16),
            pltpu.VMEM((2, line, together, features), jnp.float32),
            pltpu.VMEM((2, line, n_row - 1, share, features), jnp.float32),
            pltpu.VMEM((2, line, share, features), jnp.bfloat16),
            dma((chunks,)),
            dma,
            dma((2,)),
            dma((2, line, CORES)),
            dma((2, line)),
            dma((2, line)),
            dma((2, line)),
            dma((2, line, n_row - 1)),
            dma((2, line, n_row - 1)),
            dma((line, n_row - 1)),
            dma((line, n_row - 1)),
            dma((line,)),
            dma((2, line, line)),
            dma((2, line, per_row, n_row)),
            dma((2, line)),
            dma((2, line, per_row)),
            dma((2, line, per_row)),
        ],
        compiler_params=pltpu.CompilerParams(
            collective_id=0, has_side_effects=True, vmem_limit_bytes=62 * 2**20
        ),
        name="gather",
    )(pruned_in, dense_in, weight, keep_bits)


def tiles_kernel(tokens, panels, cols, gram, cross):
    dims = (((0,), (0,)), ((), ()))
    right = cols[...]
    for m, out in enumerate((gram, cross)):
        product = lax.dot_general(panels[m], right, dims, preferred_element_type=jnp.float32)
        out[...] = product / tokens if tokens & (tokens - 1) else product * (1.0 / tokens)


def tiles(cols, panels):
    tokens, features = cols.shape
    height = panels.shape[2]
    step = block_of(height, (256, 128))
    out = jax.ShapeDtypeStruct((height, features), jnp.float32)
    return pl.pallas_call(
        functools.partial(tiles_kernel, tokens),
        grid=(height // step,),
        out_shape=(out, out),
        in_specs=[
            pl.BlockSpec((2, tokens, step), lambda i: (0, 0, i)),
            pl.BlockSpec((tokens, features), lambda i: (0, 0)),
        ],
        out_specs=(
            pl.BlockSpec((step, features), lambda i: (i, 0)),
            pl.BlockSpec((step, features), lambda i: (i, 0)),
        ),
        name="tiles",
    )(panels, cols)


def local(dense_in, pruned_in, weight, keep_bits):
    cols, panels = gather(pruned_in, dense_in, weight, keep_bits)
    return tiles(cols, panels)


def solution(mesh):
    in_specs = (P("col", "row"), P("col", "row"), P("row", "col"), P("col", "row"))
    out_specs = (P("row", "col"), P("row", "col"))
    return jax.shard_map(local, mesh=mesh, in_specs=in_specs, out_specs=out_specs, check_vma=False)
```

```python
import functools

import jax
import jax.numpy as jnp
from jax import lax
from jax.experimental import pallas as pl
from jax.experimental.pallas import tpu as pltpu
from jax.sharding import PartitionSpec as P

MESH = pl.DeviceIdType.MESH
CORES = 2
FLAG_BITS = 16
HALF_BITS = 8
LAG = 1
PAIR_LAG = 2


def block_of(size, choices):
    for choice in choices:
        if size % choice == 0:
            return choice
    return size


def gather_kernel(
    n_row, n_col,
    pruned_in, dense_in, weight, keep,
    cols, panels,
    xs, ws, flags, pick, part, heard, posts,
    weight_sem, keep_sem, own_sem, x_recv, left_send, right_send, mate_send,
    sum_send, sum_recv, col_send, col_recv, col_own,
    post_send, post_recv, flat_send, panel_recv, pair_send, pair_recv,
):
    rows, depth = pruned_in.shape
    features = weight.shape[1]
    words = keep.shape[0]
    line = n_col // CORES
    per_row = n_col // n_row
    together = CORES * rows
    share = together // n_row
    row, col = lax.axis_index("row"), lax.axis_index("col")
    z, core = col // CORES, lax.rem(col, CORES)
    other = 1 - core
    mate = (row, z * CORES + other)

    barrier = pltpu.get_barrier_semaphore()
    signal = functools.partial(pl.semaphore_signal, barrier, inc=1, device_id_type=MESH)

    @pl.when(z > 0)
    def _():
        signal(device_id=(row, col - CORES))

    @pl.when(z < line - 1)
    def _():
        signal(device_id=(row, col + CORES))

    signal(device_id=mate)

    for d in range(1, n_row):
        signal(device_id=(lax.rem(row + d, n_row), col))

    chunk = block_of(depth, (512, 256, 128))
    chunks = depth // chunk

    def load_chunk(i):
        at = pl.ds(pl.multiple_of(i * chunk, chunk), chunk)
        return pltpu.make_async_copy(weight.at[at], ws.at[1, at], weight_sem.at[i])

    load_keep = pltpu.make_async_copy(keep, flags, keep_sem)
    load_keep.start()

    @pl.loop(0, chunks)
    def _(i):
        load_chunk(i).start()

    sources = (pruned_in, dense_in)

    def half(q, which):
        return pl.ds(pl.multiple_of(which * rows, rows), rows)

    def own_copy(m):
        return pltpu.make_async_copy(sources[m], xs.at[m, z, half(z, core)], own_sem.at[m])

    for m in range(2):
        own_copy(m).start()

    def x_copy(m, q, which, source, target, send):
        return pltpu.make_async_remote_copy(
            src_ref=source,
            dst_ref=xs.at[m, q, half(q, which)],
            send_sem=send,
            recv_sem=x_recv.at[m, q, which],
            device_id=target,
            device_id_type=MESH,
        )

    def block(m, q):
        return xs.at[m, q, half(q, core)]

    def to_left(m, q, source):
        return x_copy(m, q, core, source, (row, col - CORES), left_send.at[m, q])

    def to_right(m, q, source):
        return x_copy(m, q, core, source, (row, col + CORES), right_send.at[m, q])

    def to_mate(m, q, source):
        return x_copy(m, q, core, source, mate, mate_send.at[m, q])

    pl.semaphore_wait(barrier, 2 + n_row - jnp.where(z == 0, 1, 0) - jnp.where(z == line - 1, 1, 0))
    for m in range(2):
        @pl.when(z > 0)
        def _():
            to_left(m, z, sources[m]).start()

        @pl.when(z < line - 1)
        def _():
            to_right(m, z, sources[m]).start()

    for m in range(2):
        to_mate(m, z, sources[m]).start()

    w_at = lax.broadcasted_iota(jnp.int32, (2 * words, features), 0)
    f_at = lax.broadcasted_iota(jnp.int32, (2 * words, features), 1)
    high = jnp.where(w_at >= words, 1, 0)
    match = (w_at - high * words == f_at // FLAG_BITS) & (high == lax.rem(f_at, FLAG_BITS) // HALF_BITS)
    pick[...] = jnp.where(match, 1.0, 0.0).astype(jnp.bfloat16)
    lane = lax.broadcasted_iota(jnp.int32, (1, features), 1)
    bit = jnp.left_shift(jnp.ones_like(lane), lax.rem(lane, HALF_BITS))
    tile = block_of(chunk, (256, 128))
    load_keep.wait()

    @pl.loop(0, chunks)
    def _(i):
        load_chunk(i).wait()

        @pl.loop(0, chunk // tile)
        def _(j):
            start = pl.multiple_of(i * chunk + j * tile, tile)
            word = flags[:, pl.ds(start, tile)]
            low = (word & 255).astype(jnp.float32)
            top = (jnp.right_shift(word, HALF_BITS) & 255).astype(jnp.float32)
            halves = jnp.concatenate([low, top], 0).T.astype(jnp.bfloat16)
            spread = jnp.dot(halves, pick[...], preferred_element_type=jnp.float32)
            kept = jnp.where((spread.astype(jnp.int32) & bit) != 0, 1.0, 0.0)
            ws[0, pl.ds(start, tile), :] = ws[1, pl.ds(start, tile), :] * kept.astype(jnp.bfloat16)

    def position(s, side):
        return z + s * (1 - 2 * side)

    def present(s, side, q):
        return (q >= 0) & (q < line) & ((s > 0) | (side == 0))

    def arrive(m, s):
        @pl.loop(0, 2)
        def _(side):
            q = position(s, side)

            @pl.when(present(s, side, q) & (s > 0))
            def _():
                to_mate(m, q, block(m, q)).wait_recv()

                @pl.when((side == 0) & (z > 0))
                def _():
                    to_left(m, q, block(m, q)).start()

                @pl.when((side == 1) & (z < line - 1))
                def _():
                    to_right(m, q, block(m, q)).start()

                to_mate(m, q, block(m, q)).start()

    def sum_copy(m, q, d):
        target = lax.rem(row + d, n_row)
        at = pl.ds(pl.multiple_of(target * share, share), share)
        return pltpu.make_async_remote_copy(
            src_ref=part.at[m, q, at],
            dst_ref=heard.at[m, q, d - 1],
            send_sem=sum_send.at[m, q, d - 1],
            recv_sem=sum_recv.at[m, q, d - 1],
            device_id=(target, col),
            device_id_type=MESH,
        )

    wide = block_of(features, (512, 256, 128))

    def multiply(m, s):
        @pl.loop(0, 2)
        def _(side):
            q = position(s, side)

            @pl.when(present(s, side, q))
            def _():
                x_copy(m, q, other, block(m, q), mate, mate_send.at[m, q]).wait_recv()

                @pl.loop(0, features // wide)
                def _(n):
                    at = pl.ds(pl.multiple_of(n * wide, wide), wide)
                    part[m, q, :, at] = jnp.dot(xs[m, q], ws[m, :, at], preferred_element_type=jnp.float32)

                @pl.when(m == 1)
                def _():
                    part[1, q] = part[1, q] - part[0, q]

                for d in range(1, n_row):
                    sum_copy(m, q, d).start()

    def token_rows(q, which):
        return pl.ds(pl.multiple_of(q * together + which * share, share), share)

    def slot_columns(j):
        return pl.ds(pl.multiple_of(j * features, features), features)

    def col_copy(q, d):
        return pltpu.make_async_remote_copy(
            src_ref=posts.at[0, q, z],
            dst_ref=cols.at[token_rows(q, row)],
            send_sem=col_send.at[q, d - 1],
            recv_sem=col_recv.at[q, d - 1],
            device_id=(lax.rem(row + d, n_row), col),
            device_id_type=MESH,
        )

    def col_local(q):
        return pltpu.make_async_copy(posts.at[0, q, z], cols.at[token_rows(q, row)], col_own.at[q])

    def post_copy(m, q, f, way):
        return pltpu.make_async_remote_copy(
            src_ref=posts.at[m, q, f],
            dst_ref=posts.at[m, q, f],
            send_sem=post_send.at[way, m, q, f],
            recv_sem=post_recv.at[m, q, f],
            device_id=(row, col + CORES * (2 * way - 1)),
            device_id_type=MESH,
        )

    def can_go(way):
        return z < line - 1 if way else z > 0

    def panel_at(m, q, j, source_row):
        return panels.at[m, token_rows(q, source_row), slot_columns(j)]

    def flat_local(m, q, f):
        j = lax.rem(f * CORES + core, per_row)
        return pltpu.make_async_copy(posts.at[m, q, f], panel_at(m, q, j, row), flat_send.at[m, q, f])

    def flat_copy(m, q, f, j, source_row):
        return pltpu.make_async_remote_copy(
            src_ref=posts.at[m, q, f],
            dst_ref=panel_at(m, q, j, source_row),
            send_sem=flat_send.at[m, q, f],
            recv_sem=panel_recv.at[m, q, j, source_row],
            device_id=((f * CORES + core) // per_row, col),
            device_id_type=MESH,
        )

    def flat_own(f):
        return (f * CORES + core) // per_row == row

    def send_flat(m, q, f):
        @pl.when(flat_own(f))
        def _():
            flat_local(m, q, f).start()

        @pl.when(jnp.logical_not(flat_own(f)))
        def _():
            flat_copy(m, q, f, lax.rem(f * CORES + core, per_row), row).start()

    def send_own(t):
        s, m = t // 2, lax.rem(t, 2)

        @pl.loop(0, 2)
        def _(side):
            q = position(s, side)

            @pl.when(present(s, side, q))
            def _():
                for way in range(2):
                    @pl.when(can_go(way))
                    def _():
                        post_copy(m, q, z, way).start()

    def relay(t, d):
        s, m = t // 2, lax.rem(t, 2)
        for way in range(2):
            f = z + d * (1 - 2 * way)

            @pl.when((f >= 0) & (f < line))
            def _():
                @pl.loop(0, 2)
                def _(side):
                    q = f + s * (1 - 2 * side)

                    @pl.when(present(s, side, q))
                    def _():
                        post_copy(m, q, f, way).wait_recv()

                        @pl.when(can_go(way))
                        def _():
                            post_copy(m, q, f, way).start()

                        send_flat(m, q, f)

    def settle(m, s):
        @pl.loop(0, 2)
        def _(side):
            q = position(s, side)

            @pl.when(present(s, side, q))
            def _():
                total = part[m, q, pl.ds(pl.multiple_of(row * share, share), share), :]
                for d in range(1, n_row):
                    sum_copy(m, q, d).wait_recv()
                    total = total + heard[m, q, d - 1]
                posts[m, q, z] = total.astype(jnp.bfloat16)
                send_flat(m, q, z)

                @pl.when(m == 0)
                def _():
                    col_local(q).start()
                    for d in range(1, n_row):
                        col_copy(q, d).start()

    for m in range(2):
        own_copy(m).wait()

    last = 2 * line - 1
    at_end = (z == 0) | (z == line - 1)

    @pl.loop(0, last + 1)
    def _(t):
        s, m = t // 2, lax.rem(t, 2)

        @pl.when((t == last) & at_end)
        def _():
            @pl.loop(0, last - 1)
            def _(before):
                send_own(before)

        arrive(m, s)
        multiply(m, s)

        @pl.when(t > 0)
        def _():
            settle(1 - m, (t - 1) // 2)

    @pl.when(at_end)
    def _():
        send_own(last - 1)

    settle(1, line - 1)

    @pl.when(at_end)
    def _():
        send_own(last)

    def comes_here(j):
        return lax.rem(row * per_row + j, CORES) == core

    def panel_rows(q):
        return pl.ds(pl.multiple_of(q * together, together), together)

    def pair_copy(m, q, j):
        part_of = panels.at[m, panel_rows(q), slot_columns(j)]
        return pltpu.make_async_remote_copy(
            src_ref=part_of,
            dst_ref=part_of,
            send_sem=pair_send.at[m, q, j],
            recv_sem=pair_recv.at[m, q, j],
            device_id=mate,
            device_id_type=MESH,
        )

    def pair_up(t):
        s, m = t // 2, lax.rem(t, 2)

        @pl.loop(0, 2)
        def _(side):
            for j in range(per_row):
                origin = (row * per_row + j) // CORES
                q = origin + s * (1 - 2 * side)

                @pl.when(present(s, side, q) & comes_here(j))
                def _():
                    for source_row in range(n_row):
                        @pl.when(row == source_row)
                        def _():
                            flat_local(m, q, origin).wait()

                        @pl.when(row != source_row)
                        def _():
                            flat_copy(m, q, origin, j, source_row).wait_recv()

                    pair_copy(m, q, j).start()

    behind = LAG * (line - 1) + PAIR_LAG

    @pl.loop(0, last + 1 + behind)
    def _(u):
        @pl.when(jnp.logical_not(at_end) & (u <= last))
        def _():
            send_own(u)

        @pl.loop(1, line)
        def _(d):
            t = u - LAG * d

            @pl.when((t >= 0) & (t <= last))
            def _():
                relay(t, d)

        @pl.when(u >= behind)
        def _():
            pair_up(u - behind)

    @pl.loop(0, line)
    def _(q):
        col_local(q).wait()
        for d in range(1, n_row):
            col_copy(q, d).wait_recv()
            col_copy(q, d).wait_send()
        for m in range(2):
            for j in range(per_row):
                @pl.when(comes_here(j))
                def _():
                    pair_copy(m, q, j).wait_send()

                @pl.when(jnp.logical_not(comes_here(j)))
                def _():
                    pair_copy(m, q, j).wait_recv()

            @pl.loop(0, line)
            def _(f):
                @pl.when(jnp.logical_not(flat_own(f)))
                def _():
                    flat_copy(m, q, f, lax.rem(f * CORES + core, per_row), row).wait_send()

                @pl.when((z > 0) & (f >= z))
                def _():
                    post_copy(m, q, f, 0).wait_send()

                @pl.when((z < line - 1) & (f <= z))
                def _():
                    post_copy(m, q, f, 1).wait_send()

            for d in range(1, n_row):
                sum_copy(m, q, d).wait_send()
            to_mate(m, q, block(m, q)).wait_send()

            @pl.when((z > 0) & (q >= z))
            def _():
                to_left(m, q, block(m, q)).wait_send()

            @pl.when((z < line - 1) & (q <= z))
            def _():
                to_right(m, q, block(m, q)).wait_send()


def gather(pruned_in, dense_in, weight, keep_bits):
    n_row, n_col = lax.axis_size("row"), lax.axis_size("col")
    rows, depth = pruned_in.shape
    features = weight.shape[1]
    words = keep_bits.shape[0]
    line, per_row = n_col // CORES, n_col // n_row
    together, tokens = CORES * rows, n_col * rows
    share = together // n_row
    dma = pltpu.SemaphoreType.DMA
    chunks = depth // block_of(depth, (512, 256, 128))
    anywhere = pl.BlockSpec(memory_space=pl.ANY)
    return pl.pallas_call(
        functools.partial(gather_kernel, n_row, n_col),
        out_shape=(
            jax.ShapeDtypeStruct((tokens, features), jnp.bfloat16),
            jax.ShapeDtypeStruct((2, tokens, per_row * features), jnp.bfloat16),
        ),
        in_specs=[anywhere] * 4,
        out_specs=(anywhere, anywhere),
        scratch_shapes=[
            pltpu.VMEM((2, line, together, depth), jnp.bfloat16),
            pltpu.VMEM((2, depth, features), jnp.bfloat16),
            pltpu.VMEM((words, depth), jnp.int32),
            pltpu.VMEM((2 * words, features), jnp.bfloat16),
            pltpu.VMEM((2, line, together, features), jnp.float32),
            pltpu.VMEM((2, line, n_row - 1, share, features), jnp.float32),
            pltpu.VMEM((2, line, line, share, features), jnp.bfloat16),
            dma((chunks,)),
            dma,
            dma((2,)),
            dma((2, line, CORES)),
            dma((2, line)),
            dma((2, line)),
            dma((2, line)),
            dma((2, line, n_row - 1)),
            dma((2, line, n_row - 1)),
            dma((line, n_row - 1)),
            dma((line, n_row - 1)),
            dma((line,)),
            dma((2, 2, line, line)),
            dma((2, line, line)),
            dma((2, line, line)),
            dma((2, line, per_row, n_row)),
            dma((2, line, per_row)),
            dma((2, line, per_row)),
        ],
        compiler_params=pltpu.CompilerParams(
            collective_id=0, has_side_effects=True, vmem_limit_bytes=62 * 2**20
        ),
        name="gather",
    )(pruned_in, dense_in, weight, keep_bits)


def tiles_kernel(tokens, panels, cols, gram, cross):
    dims = (((0,), (0,)), ((), ()))
    right = cols[...]
    for m, out in enumerate((gram, cross)):
        product = lax.dot_general(panels[m], right, dims, preferred_element_type=jnp.float32)
        out[...] = product / tokens if tokens & (tokens - 1) else product * (1.0 / tokens)


def tiles(cols, panels):
    tokens, features = cols.shape
    height = panels.shape[2]
    step = block_of(height, (512, 256, 128))
    out = jax.ShapeDtypeStruct((height, features), jnp.float32)
    return pl.pallas_call(
        functools.partial(tiles_kernel, tokens),
        grid=(height // step,),
        out_shape=(out, out),
        in_specs=[
            pl.BlockSpec((2, tokens, step), lambda i: (0, 0, i)),
            pl.BlockSpec((tokens, features), lambda i: (0, 0)),
        ],
        out_specs=(
            pl.BlockSpec((step, features), lambda i: (i, 0)),
            pl.BlockSpec((step, features), lambda i: (i, 0)),
        ),
        name="tiles",
    )(panels, cols)


def local(dense_in, pruned_in, weight, keep_bits):
    cols, panels = gather(pruned_in, dense_in, weight, keep_bits)
    return tiles(cols, panels)


def solution(mesh):
    in_specs = (P("col", "row"), P("col", "row"), P("row", "col"), P("col", "row"))
    out_specs = (P("row", "col"), P("row", "col"))
    return jax.shard_map(local, mesh=mesh, in_specs=in_specs, out_specs=out_specs, check_vma=False)
```

```python
import functools

import jax
import jax.numpy as jnp
from jax import lax
from jax.experimental import pallas as pl
from jax.experimental.pallas import tpu as pltpu
from jax.sharding import PartitionSpec as P

MESH = pl.DeviceIdType.MESH
CORES = 2
FLAG_BITS = 16
HALF_BITS = 8
LAG = 1
EARLY = 3
PAIR_LAG = 2


def block_of(size, choices):
    for choice in choices:
        if size % choice == 0:
            return choice
    return size


def gather_kernel(
    n_row, n_col,
    pruned_in, dense_in, weight, keep,
    cols, panels,
    xs, ws, flags, pick, part, heard, posts,
    weight_sem, keep_sem, own_sem, x_recv, left_send, right_send, mate_send,
    sum_send, sum_recv, col_send, col_recv, col_own,
    post_send, post_recv, flat_send, panel_recv, pair_send, pair_recv,
):
    rows, depth = pruned_in.shape
    features = weight.shape[1]
    words = keep.shape[0]
    line = n_col // CORES
    per_row = n_col // n_row
    together = CORES * rows
    share = together // n_row
    row, col = lax.axis_index("row"), lax.axis_index("col")
    z, core = col // CORES, lax.rem(col, CORES)
    other = 1 - core
    mate = (row, z * CORES + other)

    barrier = pltpu.get_barrier_semaphore()
    signal = functools.partial(pl.semaphore_signal, barrier, inc=1, device_id_type=MESH)

    @pl.when(z > 0)
    def _():
        signal(device_id=(row, col - CORES))

    @pl.when(z < line - 1)
    def _():
        signal(device_id=(row, col + CORES))

    signal(device_id=mate)

    for d in range(1, n_row):
        signal(device_id=(lax.rem(row + d, n_row), col))

    chunk = block_of(depth, (512, 256, 128))
    chunks = depth // chunk

    def load_chunk(i):
        at = pl.ds(pl.multiple_of(i * chunk, chunk), chunk)
        return pltpu.make_async_copy(weight.at[at], ws.at[1, at], weight_sem.at[i])

    load_keep = pltpu.make_async_copy(keep, flags, keep_sem)
    load_keep.start()

    @pl.loop(0, chunks)
    def _(i):
        load_chunk(i).start()

    sources = (pruned_in, dense_in)

    def half(q, which):
        return pl.ds(pl.multiple_of(which * rows, rows), rows)

    def own_copy(m):
        return pltpu.make_async_copy(sources[m], xs.at[m, z, half(z, core)], own_sem.at[m])

    for m in range(2):
        own_copy(m).start()

    def x_copy(m, q, which, source, target, send):
        return pltpu.make_async_remote_copy(
            src_ref=source,
            dst_ref=xs.at[m, q, half(q, which)],
            send_sem=send,
            recv_sem=x_recv.at[m, q, which],
            device_id=target,
            device_id_type=MESH,
        )

    def block(m, q):
        return xs.at[m, q, half(q, core)]

    def to_left(m, q, source):
        return x_copy(m, q, core, source, (row, col - CORES), left_send.at[m, q])

    def to_right(m, q, source):
        return x_copy(m, q, core, source, (row, col + CORES), right_send.at[m, q])

    def to_mate(m, q, source):
        return x_copy(m, q, core, source, mate, mate_send.at[m, q])

    pl.semaphore_wait(barrier, 2 + n_row - jnp.where(z == 0, 1, 0) - jnp.where(z == line - 1, 1, 0))
    for m in range(2):
        @pl.when(z > 0)
        def _():
            to_left(m, z, sources[m]).start()

        @pl.when(z < line - 1)
        def _():
            to_right(m, z, sources[m]).start()

    for m in range(2):
        to_mate(m, z, sources[m]).start()

    w_at = lax.broadcasted_iota(jnp.int32, (2 * words, features), 0)
    f_at = lax.broadcasted_iota(jnp.int32, (2 * words, features), 1)
    high = jnp.where(w_at >= words, 1, 0)
    match = (w_at - high * words == f_at // FLAG_BITS) & (high == lax.rem(f_at, FLAG_BITS) // HALF_BITS)
    pick[...] = jnp.where(match, 1.0, 0.0).astype(jnp.bfloat16)
    lane = lax.broadcasted_iota(jnp.int32, (1, features), 1)
    bit = jnp.left_shift(jnp.ones_like(lane), lax.rem(lane, HALF_BITS))
    tile = block_of(chunk, (256, 128))
    load_keep.wait()

    @pl.loop(0, chunks)
    def _(i):
        load_chunk(i).wait()

        @pl.loop(0, chunk // tile)
        def _(j):
            start = pl.multiple_of(i * chunk + j * tile, tile)
            word = flags[:, pl.ds(start, tile)]
            low = (word & 255).astype(jnp.float32)
            top = (jnp.right_shift(word, HALF_BITS) & 255).astype(jnp.float32)
            halves = jnp.concatenate([low, top], 0).T.astype(jnp.bfloat16)
            spread = jnp.dot(halves, pick[...], preferred_element_type=jnp.float32)
            kept = jnp.where((spread.astype(jnp.int32) & bit) != 0, 1.0, 0.0)
            ws[0, pl.ds(start, tile), :] = ws[1, pl.ds(start, tile), :] * kept.astype(jnp.bfloat16)

    def position(s, side):
        return z + s * (1 - 2 * side)

    def present(s, side, q):
        return (q >= 0) & (q < line) & ((s > 0) | (side == 0))

    def arrive(m, s):
        @pl.loop(0, 2)
        def _(side):
            q = position(s, side)

            @pl.when(present(s, side, q) & (s > 0))
            def _():
                to_mate(m, q, block(m, q)).wait_recv()

                @pl.when((side == 0) & (z > 0))
                def _():
                    to_left(m, q, block(m, q)).start()

                @pl.when((side == 1) & (z < line - 1))
                def _():
                    to_right(m, q, block(m, q)).start()

                to_mate(m, q, block(m, q)).start()

    def sum_copy(m, q, d):
        target = lax.rem(row + d, n_row)
        at = pl.ds(pl.multiple_of(target * share, share), share)
        return pltpu.make_async_remote_copy(
            src_ref=part.at[m, q, at],
            dst_ref=heard.at[m, q, d - 1],
            send_sem=sum_send.at[m, q, d - 1],
            recv_sem=sum_recv.at[m, q, d - 1],
            device_id=(target, col),
            device_id_type=MESH,
        )

    wide = block_of(features, (512, 256, 128))

    def multiply(m, s):
        @pl.loop(0, 2)
        def _(side):
            q = position(s, side)

            @pl.when(present(s, side, q))
            def _():
                x_copy(m, q, other, block(m, q), mate, mate_send.at[m, q]).wait_recv()

                @pl.loop(0, features // wide)
                def _(n):
                    at = pl.ds(pl.multiple_of(n * wide, wide), wide)
                    part[m, q, :, at] = jnp.dot(xs[m, q], ws[m, :, at], preferred_element_type=jnp.float32)

                @pl.when(m == 1)
                def _():
                    part[1, q] = part[1, q] - part[0, q]

                for d in range(1, n_row):
                    sum_copy(m, q, d).start()

    def token_rows(q, which):
        return pl.ds(pl.multiple_of(q * together + which * share, share), share)

    def slot_columns(j):
        return pl.ds(pl.multiple_of(j * features, features), features)

    def col_copy(q, d):
        return pltpu.make_async_remote_copy(
            src_ref=posts.at[0, q, z],
            dst_ref=cols.at[token_rows(q, row)],
            send_sem=col_send.at[q, d - 1],
            recv_sem=col_recv.at[q, d - 1],
            device_id=(lax.rem(row + d, n_row), col),
            device_id_type=MESH,
        )

    def col_local(q):
        return pltpu.make_async_copy(posts.at[0, q, z], cols.at[token_rows(q, row)], col_own.at[q])

    def post_copy(m, q, f, way):
        return pltpu.make_async_remote_copy(
            src_ref=posts.at[m, q, f],
            dst_ref=posts.at[m, q, f],
            send_sem=post_send.at[way, m, q, f],
            recv_sem=post_recv.at[m, q, f],
            device_id=(row, col + CORES * (2 * way - 1)),
            device_id_type=MESH,
        )

    def can_go(way):
        return z < line - 1 if way else z > 0

    def panel_at(m, q, j, source_row):
        return panels.at[m, token_rows(q, source_row), slot_columns(j)]

    def flat_local(m, q, f):
        j = lax.rem(f * CORES + core, per_row)
        return pltpu.make_async_copy(posts.at[m, q, f], panel_at(m, q, j, row), flat_send.at[m, q, f])

    def flat_copy(m, q, f, j, source_row):
        return pltpu.make_async_remote_copy(
            src_ref=posts.at[m, q, f],
            dst_ref=panel_at(m, q, j, source_row),
            send_sem=flat_send.at[m, q, f],
            recv_sem=panel_recv.at[m, q, j, source_row],
            device_id=((f * CORES + core) // per_row, col),
            device_id_type=MESH,
        )

    def flat_own(f):
        return (f * CORES + core) // per_row == row

    def send_flat(m, q, f):
        @pl.when(flat_own(f))
        def _():
            flat_local(m, q, f).start()

        @pl.when(jnp.logical_not(flat_own(f)))
        def _():
            flat_copy(m, q, f, lax.rem(f * CORES + core, per_row), row).start()

    def send_own(t):
        s, m = t // 2, lax.rem(t, 2)

        @pl.loop(0, 2)
        def _(side):
            q = position(s, side)

            @pl.when(present(s, side, q))
            def _():
                for way in range(2):
                    @pl.when(can_go(way))
                    def _():
                        post_copy(m, q, z, way).start()

    def relay(t, d):
        s, m = t // 2, lax.rem(t, 2)
        for way in range(2):
            f = z + d * (1 - 2 * way)

            @pl.when((f >= 0) & (f < line))
            def _():
                @pl.loop(0, 2)
                def _(side):
                    q = f + s * (1 - 2 * side)

                    @pl.when(present(s, side, q))
                    def _():
                        post_copy(m, q, f, way).wait_recv()

                        @pl.when(can_go(way))
                        def _():
                            post_copy(m, q, f, way).start()

                        send_flat(m, q, f)

    def settle(m, s):
        @pl.loop(0, 2)
        def _(side):
            q = position(s, side)

            @pl.when(present(s, side, q))
            def _():
                total = part[m, q, pl.ds(pl.multiple_of(row * share, share), share), :]
                for d in range(1, n_row):
                    sum_copy(m, q, d).wait_recv()
                    total = total + heard[m, q, d - 1]
                posts[m, q, z] = total.astype(jnp.bfloat16)
                send_flat(m, q, z)

                @pl.when(m == 0)
                def _():
                    col_local(q).start()
                    for d in range(1, n_row):
                        col_copy(q, d).start()

    for m in range(2):
        own_copy(m).wait()

    last = 2 * line - 1
    at_end = (z == 0) | (z == line - 1)

    @pl.loop(0, last + 1)
    def _(t):
        s, m = t // 2, lax.rem(t, 2)

        @pl.when((t == last) & at_end)
        def _():
            @pl.loop(0, last - 1)
            def _(before):
                send_own(before)

        arrive(m, s)
        multiply(m, s)

        @pl.when(t > 0)
        def _():
            settle(1 - m, (t - 1) // 2)

    @pl.when(at_end)
    def _():
        send_own(last - 1)


    def comes_here(j):
        return lax.rem(row * per_row + j, CORES) == core

    def panel_rows(q):
        return pl.ds(pl.multiple_of(q * together, together), together)

    def pair_copy(m, q, j):
        part_of = panels.at[m, panel_rows(q), slot_columns(j)]
        return pltpu.make_async_remote_copy(
            src_ref=part_of,
            dst_ref=part_of,
            send_sem=pair_send.at[m, q, j],
            recv_sem=pair_recv.at[m, q, j],
            device_id=mate,
            device_id_type=MESH,
        )

    def pair_up(t):
        s, m = t // 2, lax.rem(t, 2)

        @pl.loop(0, 2)
        def _(side):
            for j in range(per_row):
                origin = (row * per_row + j) // CORES
                q = origin + s * (1 - 2 * side)

                @pl.when(present(s, side, q) & comes_here(j))
                def _():
                    for source_row in range(n_row):
                        @pl.when(row == source_row)
                        def _():
                            flat_local(m, q, origin).wait()

                        @pl.when(row != source_row)
                        def _():
                            flat_copy(m, q, origin, j, source_row).wait_recv()

                    pair_copy(m, q, j).start()

    behind = LAG * (line - 1) + PAIR_LAG

    def advance(u):
        @pl.when(jnp.logical_not(at_end) & (u <= last))
        def _():
            send_own(u)

        @pl.loop(1, line)
        def _(d):
            t = u - LAG * d

            @pl.when((t >= 0) & (t <= last))
            def _():
                relay(t, d)

        @pl.when(u >= behind)
        def _():
            pair_up(u - behind)

    @pl.loop(0, EARLY)
    def _(u):
        advance(u)

    settle(1, line - 1)

    @pl.when(at_end)
    def _():
        send_own(last)

    @pl.loop(EARLY, last + 1 + behind)
    def _(u):
        advance(u)

    @pl.loop(0, line)
    def _(q):
        col_local(q).wait()
        for d in range(1, n_row):
            col_copy(q, d).wait_recv()
            col_copy(q, d).wait_send()
        for m in range(2):
            for j in range(per_row):
                @pl.when(comes_here(j))
                def _():
                    pair_copy(m, q, j).wait_send()

                @pl.when(jnp.logical_not(comes_here(j)))
                def _():
                    pair_copy(m, q, j).wait_recv()

            @pl.loop(0, line)
            def _(f):
                @pl.when(jnp.logical_not(flat_own(f)))
                def _():
                    flat_copy(m, q, f, lax.rem(f * CORES + core, per_row), row).wait_send()

                @pl.when((z > 0) & (f >= z))
                def _():
                    post_copy(m, q, f, 0).wait_send()

                @pl.when((z < line - 1) & (f <= z))
                def _():
                    post_copy(m, q, f, 1).wait_send()

            for d in range(1, n_row):
                sum_copy(m, q, d).wait_send()
            to_mate(m, q, block(m, q)).wait_send()

            @pl.when((z > 0) & (q >= z))
            def _():
                to_left(m, q, block(m, q)).wait_send()

            @pl.when((z < line - 1) & (q <= z))
            def _():
                to_right(m, q, block(m, q)).wait_send()


def gather(pruned_in, dense_in, weight, keep_bits):
    n_row, n_col = lax.axis_size("row"), lax.axis_size("col")
    rows, depth = pruned_in.shape
    features = weight.shape[1]
    words = keep_bits.shape[0]
    line, per_row = n_col // CORES, n_col // n_row
    together, tokens = CORES * rows, n_col * rows
    share = together // n_row
    dma = pltpu.SemaphoreType.DMA
    chunks = depth // block_of(depth, (512, 256, 128))
    anywhere = pl.BlockSpec(memory_space=pl.ANY)
    return pl.pallas_call(
        functools.partial(gather_kernel, n_row, n_col),
        out_shape=(
            jax.ShapeDtypeStruct((tokens, features), jnp.bfloat16),
            jax.ShapeDtypeStruct((2, tokens, per_row * features), jnp.bfloat16),
        ),
        in_specs=[anywhere] * 4,
        out_specs=(anywhere, anywhere),
        scratch_shapes=[
            pltpu.VMEM((2, line, together, depth), jnp.bfloat16),
            pltpu.VMEM((2, depth, features), jnp.bfloat16),
            pltpu.VMEM((words, depth), jnp.int32),
            pltpu.VMEM((2 * words, features), jnp.bfloat16),
            pltpu.VMEM((2, line, together, features), jnp.float32),
            pltpu.VMEM((2, line, n_row - 1, share, features), jnp.float32),
            pltpu.VMEM((2, line, line, share, features), jnp.bfloat16),
            dma((chunks,)),
            dma,
            dma((2,)),
            dma((2, line, CORES)),
            dma((2, line)),
            dma((2, line)),
            dma((2, line)),
            dma((2, line, n_row - 1)),
            dma((2, line, n_row - 1)),
            dma((line, n_row - 1)),
            dma((line, n_row - 1)),
            dma((line,)),
            dma((2, 2, line, line)),
            dma((2, line, line)),
            dma((2, line, line)),
            dma((2, line, per_row, n_row)),
            dma((2, line, per_row)),
            dma((2, line, per_row)),
        ],
        compiler_params=pltpu.CompilerParams(
            collective_id=0, has_side_effects=True, vmem_limit_bytes=62 * 2**20
        ),
        name="gather",
    )(pruned_in, dense_in, weight, keep_bits)


def tiles_kernel(tokens, panels, cols, gram, cross):
    dims = (((0,), (0,)), ((), ()))
    right = cols[...]
    for m, out in enumerate((gram, cross)):
        product = lax.dot_general(panels[m], right, dims, preferred_element_type=jnp.float32)
        out[...] = product / tokens if tokens & (tokens - 1) else product * (1.0 / tokens)


def tiles(cols, panels):
    tokens, features = cols.shape
    height = panels.shape[2]
    step = block_of(height, (512, 256, 128))
    out = jax.ShapeDtypeStruct((height, features), jnp.float32)
    return pl.pallas_call(
        functools.partial(tiles_kernel, tokens),
        grid=(height // step,),
        out_shape=(out, out),
        in_specs=[
            pl.BlockSpec((2, tokens, step), lambda i: (0, 0, i)),
            pl.BlockSpec((tokens, features), lambda i: (0, 0)),
        ],
        out_specs=(
            pl.BlockSpec((step, features), lambda i: (i, 0)),
            pl.BlockSpec((step, features), lambda i: (i, 0)),
        ),
        name="tiles",
    )(panels, cols)


def local(dense_in, pruned_in, weight, keep_bits):
    cols, panels = gather(pruned_in, dense_in, weight, keep_bits)
    return tiles(cols, panels)


def solution(mesh):
    in_specs = (P("col", "row"), P("col", "row"), P("row", "col"), P("col", "row"))
    out_specs = (P("row", "col"), P("row", "col"))
    return jax.shard_map(local, mesh=mesh, in_specs=in_specs, out_specs=out_specs, check_vma=False)
```
